512 devices in a mesh: grp: 4 (over x), row: 16 (over z, core), col: 8 (over y).
Axes of the slice: x: 4, y: 8, z: 8, core: 2. Of those that a mesh axis runs over, the one named last changes fastest.
Arguments:
- fields: bfloat16 [4, 4, 768, 6144], P('grp', None, 'row', 'col'), may hold values from -12 to 12
- offset: int32 [1], replicated, may hold values from 0 to 767
- level_index: int32 [4], replicated, may hold values from 0 to 3, each once
- nudge_rate: float32 [4], replicated, may hold values from 0.2 to 0.9
- driving: float32 [4, 64, 64], replicated, may hold values from -4 to 4
Outputs:
- nudged: bfloat16 [4, 4, 768, 6144], P('grp', None, 'row', 'col')
The draws below stay inside these ranges and needn't reach their ends.
Inputs may be any that keep to these rules, and one draw needn't show every extreme that they name: `offset`: the footprint covers a third of the parent rows from there on, wrapping around the periodic domain. `level_index`: each parent level is fed by exactly one child level.
All inputs are finite; a program needn't handle non-finite values.
Results may differ from the reference program's by a relative error of at most 0.0034.
Values may be sent and summed in bfloat16 or wider, within the bound.
A program may use at most 64 MiB of HBM per device.

```python
import math
import jax
import jax.numpy as jnp
from jax import lax

LEVELS = 4
TILE_COLS = 768
MAX_WAVE = 32
BASIS = 64
PARENT_ROWS = 768
PARENT_COLS = 6144
N_GRP = 4


def fourier_table_drawn(positions, cell_count, max_order):
    orders = jnp.arange(1, max_order + 1, dtype=jnp.int32)
    period = 3 * cell_count
    phase_index = positions[:, None] * orders[None, :] % period
    angles = phase_index.astype(jnp.float32) * jnp.float32(2.0 * math.pi / period)
    wave_scale = jnp.float32(math.sqrt(2.0 / cell_count))
    constant = jnp.full((positions.shape[0], 1), 1.0 / math.sqrt(cell_count), jnp.float32)
    return jnp.concatenate([constant, wave_scale * jnp.cos(angles), wave_scale * jnp.sin(angles[:, :max_order - 1])], axis=1)


def draw_fields(key, part):
    key_noise = jax.random.fold_in(key, 11)
    key_parent = jax.random.fold_in(key, 12)
    key_child = jax.random.fold_in(key, 13)
    amplitude = math.sqrt(PARENT_ROWS * PARENT_COLS) / BASIS
    row_ids = jnp.arange(PARENT_ROWS, dtype=jnp.int32)
    col_ids = jnp.arange(PARENT_COLS, dtype=jnp.int32)
    row_table = fourier_table_drawn(3 * row_ids, PARENT_ROWS, MAX_WAVE)
    col_table = fourier_table_drawn(3 * col_ids, PARENT_COLS, MAX_WAVE)
    child_row_table = fourier_table_drawn((row_ids - 1) % (3 * PARENT_ROWS), PARENT_ROWS, MAX_WAVE)
    tile_ids = col_ids // TILE_COLS
    within = col_ids % TILE_COLS
    child_col_tables = jnp.stack([fourier_table_drawn(((3 * tile_ids + slot) * TILE_COLS + within - 1) % (3 * PARENT_COLS), PARENT_COLS, MAX_WAVE) for slot in range(3)])
    shape = (N_GRP, LEVELS, PARENT_ROWS, PARENT_COLS)
    noise_part = jax.random.normal(key_noise, shape, jnp.float32)
    parent_coef = jax.random.normal(key_parent, (LEVELS, BASIS, BASIS), jnp.float32) * amplitude
    child_coef = jax.random.normal(key_child, (LEVELS, BASIS, BASIS), jnp.float32) * amplitude
    parent_cols = jnp.einsum('lnm,jm->lnj', parent_coef, col_table)
    parent_smooth = jnp.einsum('in,lnj->lij', row_table, parent_cols)
    child_cols = jnp.einsum('lnm,gjm->glnj', child_coef, child_col_tables)
    child_smooth = jnp.einsum('in,glnj->glij', child_row_table, child_cols)
    smooth_part = jnp.concatenate([child_smooth, parent_smooth[None]], axis=0)
    total = jnp.clip(smooth_part + noise_part, -12.0, 12.0)
    return total.astype(jnp.bfloat16)


def noise(own_key, shape, scale, most, held_as=jnp.bfloat16):
    return jnp.clip(scale * jax.random.normal(own_key, shape, jnp.float32), -most, most).astype(held_as)


def setup_inputs(seed: int = 0) -> dict:
    key_of = jax.random.split(jax.random.key(seed), 6)
    fields = draw_fields(jax.random.fold_in(key_of[5], 71), 0)
    offset = jax.random.randint(key_of[1], (1,), 0, PARENT_ROWS).astype(jnp.int32)
    level_index = jax.random.permutation(key_of[2], LEVELS).astype(jnp.int32)
    nudge_rate = jnp.clip(jnp.exp(jax.random.uniform(key_of[3], (LEVELS,), jnp.float32, math.log(0.2), math.log(0.9))), 0.2, 0.9)
    driving = noise(key_of[4], (LEVELS, BASIS, BASIS), 1.0, 4.0, jnp.float32)
    return {"fields": fields, "offset": offset, "level_index": level_index, "nudge_rate": nudge_rate, "driving": driving}


def fourier_table(positions, cell_count, max_order):
    orders = jnp.arange(1, max_order + 1, dtype=jnp.int32)
    period = 3 * cell_count
    phase_index = positions[:, None] * orders[None, :] % period
    angles = phase_index.astype(jnp.float32) * jnp.float32(2.0 * math.pi / period)
    wave_scale = jnp.float32(math.sqrt(2.0 / cell_count))
    constant = jnp.full((positions.shape[0], 1), 1.0 / math.sqrt(cell_count), jnp.float32)
    return jnp.concatenate([constant, wave_scale * jnp.cos(angles), wave_scale * jnp.sin(angles[:, :max_order - 1])], axis=1)

def reference(fields, offset, level_index, nudge_rate, driving):
    shift_rows = offset[0]
    level_ids = jnp.arange(LEVELS, dtype=jnp.int32)
    inverse = lax.optimization_barrier(jnp.sum(level_ids[:, None] * (level_index[:, None] == level_ids[None, :]).astype(jnp.int32), axis=0))
    row_ids = jnp.arange(PARENT_ROWS, dtype=jnp.int32)
    col_ids = jnp.arange(PARENT_COLS, dtype=jnp.int32)
    row_table = fourier_table(3 * row_ids, PARENT_ROWS, MAX_WAVE)
    col_table = fourier_table(3 * col_ids, PARENT_COLS, MAX_WAVE)
    row_half = lax.optimization_barrier(row_table.astype(jnp.bfloat16))
    row_rounded = row_half.astype(jnp.float32)
    col_rounded = col_table.astype(jnp.bfloat16)
    child_row_table = fourier_table((3 * shift_rows + row_ids - 1) % (3 * PARENT_ROWS), PARENT_ROWS, MAX_WAVE)
    tile_ids = col_ids // TILE_COLS
    within = col_ids % TILE_COLS
    child_col_tables = jnp.stack([fourier_table(((3 * tile_ids + slot) * TILE_COLS + within - 1) % (3 * PARENT_COLS), PARENT_COLS, MAX_WAVE) for slot in range(3)])
    amplitude = math.sqrt(PARENT_ROWS * PARENT_COLS) / BASIS
    strip_index = (row_ids - shift_rows) % PARENT_ROWS
    covered = strip_index < PARENT_ROWS // 3
    strip_rows = jnp.clip(strip_index, 0, PARENT_ROWS // 3 - 1)

    def one_level(parent_level):
        child_level = inverse[parent_level]
        child_slots = lax.dynamic_index_in_dim(fields[:N_GRP - 1], child_level, axis=1, keepdims=False)
        parent = lax.dynamic_index_in_dim(fields[N_GRP - 1], parent_level, axis=0, keepdims=False)
        block_sums = lax.optimization_barrier(jnp.sum(child_slots.reshape(3, PARENT_ROWS // 3, 3, PARENT_COLS // 3, 3), axis=(2, 4), dtype=jnp.float32))
        averaged = (block_sums / 9.0).astype(jnp.bfloat16)
        averaged = averaged.reshape(3, PARENT_ROWS // 3, PARENT_COLS // TILE_COLS, TILE_COLS // 3)
        averaged = jnp.transpose(averaged, (1, 2, 0, 3)).reshape(PARENT_ROWS // 3, PARENT_COLS)
        fed_tile = jnp.where(covered[:, None], averaged[strip_rows], parent)
        projected = jnp.dot(fed_tile, col_rounded, preferred_element_type=jnp.float32)
        coeffs = jnp.dot(row_rounded.T, projected, precision=lax.Precision.HIGHEST)
        deficit = amplitude * driving[parent_level] - coeffs
        rate = nudge_rate[parent_level]
        spread_cols = jnp.dot(deficit, col_table.T, precision=lax.Precision.HIGHEST)
        increment = jnp.dot(row_table, spread_cols, precision=lax.Precision.HIGHEST)
        parent_new = (fed_tile.astype(jnp.float32) + rate * increment).astype(jnp.bfloat16)
        child_spread = jnp.einsum('nm,gjm->gnj', deficit, child_col_tables, precision=lax.Precision.HIGHEST)
        child_increment = jnp.einsum('in,gnj->gij', child_row_table, child_spread, precision=lax.Precision.HIGHEST)
        child_new = (child_slots.astype(jnp.float32) + rate * child_increment).astype(jnp.bfloat16)
        return (parent_new, child_new)
    parents, children = lax.map(one_level, level_ids)
    children = jnp.take(children, level_index, axis=0)
    children = jnp.transpose(children, (1, 0, 2, 3))
    return jnp.concatenate([children, parents[None]], axis=0)
```

```python
import math

import jax
import jax.numpy as jnp
from jax import lax
from jax.experimental import pallas as pl
from jax.experimental.pallas import tpu as pltpu
from jax.sharding import PartitionSpec as P

MESH = pl.DeviceIdType.MESH
F32 = jnp.float32
BF16 = jnp.bfloat16
I32 = jnp.int32

L = 4
W = 32
B = 64
ROWS = 768
COLS = 6144
TR = 48
TC = 768
NX = 4
NY = 8
NZ = 8
NR = 16


def iota(shape, dim):
    return lax.broadcasted_iota(I32, shape, dim)


def basis(m, z, cells):
    period = 3 * cells
    wave = jnp.where(m <= W, m, m - W).astype(F32)
    shift = jnp.where(m <= W, 0.0, period / 4).astype(F32)
    scale = jnp.where(m == 0, 1.0 / math.sqrt(cells), math.sqrt(2.0 / cells)).astype(F32)
    phase = wave * z.astype(F32) - shift
    phase = phase - period * jnp.floor(phase * (1.0 / period))
    t = (jnp.abs(phase - period / 2) - period / 4) * (2.0 * math.pi / period)
    s = t * t
    acc = F32(1.0 / math.factorial(13))
    for k in (11, 9, 7, 5, 3, 1):
        sign = -1.0 if k in (11, 7, 3) else 1.0
        acc = acc * s + F32(sign / math.factorial(k))
    return scale * (t * acc)


def split(v):
    hi = v.astype(BF16)
    return hi, (v - hi.astype(F32)).astype(BF16)


def dot(a, b):
    return jnp.dot(a, b, preferred_element_type=F32)


def dot_nt(a, b):
    return lax.dot_general(a, b, (((1,), (1,)), ((), ())), preferred_element_type=F32)


def bytes_wait(ref, sem):
    pltpu.make_async_copy(ref, ref, sem).wait()


def kernel(
    x_hbm, off_ref, lev_ref, rate_ref, drv_ref, out_ref,
    x_ref, pool_ref, sums_ref, avg_ref, own_ref, colt_ref, part_ref, rs_ref, ysrc_ref, y_ref,
    zsrc_ref, z_ref, all_ref, gat_ref, win_ref, fed_ref, drvp_ref, rows3_ref, chi_ref, clo_ref,
    in_sem, rs_send, rs_recv, y_send, y_recv, z_send, z_recv, ag_send, ag_recv,
    g_send, g_recv, w_send, w_recv,
):
    grp = lax.axis_index("grp")
    row = lax.axis_index("row")
    col = lax.axis_index("col")
    zed = row // 2
    core = row % 2
    seat = grp * 2 + core
    is_parent = grp == NX - 1
    off = off_ref[0]

    load = pltpu.make_async_copy(x_hbm, x_ref, in_sem)
    load.start()

    barrier = pltpu.get_barrier_semaphore()

    def seat_peer(d):
        other = (seat + d) % 8
        return other, (other // 2, zed * 2 + other % 2, col)

    def y_peer(d):
        return (grp, row, (col + d) % NY)

    def z_peer(d):
        return (grp, ((zed + d) % NZ) * 2 + core, col)

    def greet(dev):
        pl.semaphore_signal(barrier, inc=1, device_id=dev, device_id_type=MESH)

    for d in range(1, 8):
        greet(seat_peer(d)[1])
        greet(y_peer(d))
        greet(z_peer(d))

    @pl.when(jnp.logical_not(is_parent))
    def _():
        for d in range(1, 8):
            greet((grp, ((zed + d) % NZ) * 2 + 1 - core, col))

    @pl.when(jnp.logical_not(is_parent))
    def _():
        j = iota((TC, 256), 0)
        t = iota((TC, 256), 1) * 3
        pool_ref[...] = jnp.where((j >= t) & (j < t + 3), 1.0, 0.0).astype(BF16)
        xs = 3 * (col * TC + grp * 256 + iota((B, 256), 1))
        colt_ref[:, :256] = basis(iota((B, 256), 0), xs, COLS).astype(BF16)

    @pl.when(is_parent)
    def _():
        xs = 3 * (col * TC + iota((B, TC), 1))
        colt_ref[...] = basis(iota((B, TC), 0), xs, COLS).astype(BF16)

    load.wait()

    def add_part(rowt, proj, rows):
        for pair in range(2):
            lo = 2 * pair * rows
            both = jnp.concatenate([proj[lo : lo + rows], proj[lo + rows : lo + 2 * rows]], axis=1)
            hi, low = split(both)
            part = dot(rowt, hi) + dot(rowt, low)
            part_ref[4 * pair : 4 * pair + 4] = part.reshape(4, 16, 128)

    @pl.when(jnp.logical_not(is_parent))
    def _():
        xs = x_ref[...].reshape(L * TR, TC)
        for h in range(2):
            cut = slice(128 * h, 128 * h + 128)
            sums_ref[h] = dot(xs, pool_ref[:, cut])
            total = (
                sums_ref[h, pl.ds(0, 64, stride=3), :]
                + sums_ref[h, pl.ds(1, 64, stride=3), :]
                + sums_ref[h, pl.ds(2, 64, stride=3), :]
            )
            avg_ref[:, :, cut] = (total / 9.0).reshape(L, 16, 128)
        for p in range(L):
            inv = jnp.int32(0)
            for l in range(1, L):
                inv = jnp.where(lev_ref[l] == p, l, inv)
            own_ref[p] = avg_ref[inv].astype(BF16)
        proj = dot_nt(own_ref[...].reshape(64, 256), colt_ref[:, :256])
        rr = off + 16 * row + iota((B, 16), 1)
        rowt = basis(iota((B, 16), 0), 3 * rr, ROWS).astype(BF16)
        add_part(rowt, proj, 16)

    @pl.when(is_parent)
    def _():
        proj = dot_nt(x_ref[...].reshape(L * TR, TC), colt_ref[...])
        rr = TR * row + iota((B, TR), 1)
        s = rr - off
        s = jnp.where(s < 0, s + ROWS, s)
        rowt = basis(iota((B, TR), 0), 3 * rr, ROWS)
        rowt = jnp.where(s < ROWS // 3, 0.0, rowt).astype(BF16)
        add_part(rowt, proj, TR)

    pl.semaphore_wait(barrier, jnp.where(is_parent, 21, 28))

    for d in range(1, 8):
        other, dev = seat_peer(d)
        pltpu.make_async_remote_copy(
            src_ref=part_ref.at[other], dst_ref=rs_ref.at[d - 1], send_sem=rs_send, recv_sem=rs_recv,
            device_id=dev, device_id_type=MESH,
        ).start()

    @pl.when(jnp.logical_not(is_parent))
    def _():
        for d in range(1, NR):
            other = (row + d) % NR
            pltpu.make_async_remote_copy(
                src_ref=own_ref.at[pl.ds(2 * (other % 2), 2)], dst_ref=gat_ref.at[row],
                send_sem=g_send, recv_sem=g_recv, device_id=(grp, other, col), device_id_type=MESH,
            ).start()
        gat_ref[row] = own_ref[pl.ds(2 * core, 2)]

    for pair in range(2):
        both = jnp.concatenate([drv_ref[2 * pair], drv_ref[2 * pair + 1]], axis=1)
        drvp_ref[4 * pair : 4 * pair + 4] = (
            both * (math.sqrt(ROWS * COLS) / (2 * W))
        ).reshape(4, 16, 128)
    t = iota((TR, B), 0)
    zr = jnp.where(is_parent, 3 * (TR * row + t), 3 * off + TR * row + t - 1)
    hi, low = split(basis(iota((TR, B), 1), zr, ROWS))
    rows3_ref[...] = jnp.concatenate([hi, hi, low], axis=1)

    bytes_wait(rs_ref, rs_recv)
    total = part_ref[seat]
    for d in range(7):
        total = total + rs_ref[d]
    ysrc_ref[...] = total
    for d in range(1, NY):
        pltpu.make_async_remote_copy(
            src_ref=ysrc_ref, dst_ref=y_ref.at[d - 1], send_sem=y_send, recv_sem=y_recv,
            device_id=y_peer(d), device_id_type=MESH,
        ).start()

    for n in range(3):
        t = iota((B, 256), 1) + 256 * n
        zc = jnp.where(is_parent, 3 * (col * TC + t), (3 * col + grp) * TC + t - 1)
        hi, low = split(basis(iota((B, 256), 0), zc, COLS))
        for p in range(L):
            chi_ref[p * B : (p + 1) * B, n * 256 : (n + 1) * 256] = hi
            clo_ref[p * B : (p + 1) * B, n * 256 : (n + 1) * 256] = low

    @pl.when(is_parent)
    def _():
        s = TR * row + iota((TR, TC), 0) - off
        s = jnp.where(s < 0, s + ROWS, s)
        for p in range(L):
            x_ref[p] = jnp.where(s < ROWS // 3, 0.0, x_ref[p].astype(F32)).astype(BF16)

    bytes_wait(y_ref, y_recv)
    total = ysrc_ref[...]
    for d in range(7):
        total = total + y_ref[d]
    zsrc_ref[...] = total
    for d in range(1, NZ):
        pltpu.make_async_remote_copy(
            src_ref=zsrc_ref, dst_ref=z_ref.at[d - 1], send_sem=z_send, recv_sem=z_recv,
            device_id=z_peer(d), device_id_type=MESH,
        ).start()

    @pl.when(jnp.logical_not(is_parent))
    def _():
        bytes_wait(gat_ref.at[pl.ds(0, NR - 1)], g_recv)
        v = 2 * TR * zed + iota((2 * TR, 256), 0) - off
        q = iota((2 * TR, 256), 1)
        pick = jnp.where((v == q) | (v + ROWS == q), 1.0, 0.0).astype(BF16)
        for k in range(2):
            rows = dot(pick, gat_ref[:, k].reshape(256, 256)).astype(BF16)
            win_ref[0, k] = rows[:TR]
            win_ref[1, k] = rows[TR:]
        for k in range(2):
            pltpu.make_async_remote_copy(
                src_ref=win_ref.at[k], dst_ref=fed_ref.at[grp, core], send_sem=w_send, recv_sem=w_recv,
                device_id=(NX - 1, 2 * zed + k, col), device_id_type=MESH,
            ).start()

    bytes_wait(z_ref, z_recv)
    total = zsrc_ref[...]
    for d in range(7):
        total = total + z_ref[d]
    all_ref[seat] = drvp_ref[seat] - total
    for d in range(1, 8):
        pltpu.make_async_remote_copy(
            src_ref=all_ref.at[seat], dst_ref=all_ref.at[seat], send_sem=ag_send, recv_sem=ag_recv,
            device_id=seat_peer(d)[1], device_id_type=MESH,
        ).start()
    bytes_wait(all_ref.at[pl.ds(0, 7)], ag_recv)

    hi, low = split(
        jnp.concatenate([all_ref[0:4].reshape(B, 128), all_ref[4:8].reshape(B, 128)], axis=1)
    )
    left = dot(rows3_ref[...], jnp.concatenate([hi, low, hi], axis=0))
    slot = iota((TR, 256), 1) // B
    parts = []
    for l in range(L):
        lev = jnp.where(is_parent, l, lev_ref[l])
        parts.append(jnp.where(slot == lev, left * rate_ref[lev], 0.0))
    lhi, llow = split(jnp.concatenate(parts, axis=0))

    @pl.when(is_parent)
    def _():
        bytes_wait(fed_ref, w_recv)
        for g in range(3):
            for p in range(L):
                cut = (p, slice(None), slice(256 * g, 256 * g + 256))
                x_ref[cut] = x_ref[cut] + fed_ref[g, p // 2, p % 2]

    for n in range(3):
        cut = slice(n * 256, n * 256 + 256)
        inc = dot(lhi, chi_ref[:, cut]) + dot(lhi, clo_ref[:, cut]) + dot(llow, chi_ref[:, cut])
        base = x_ref[:, :, cut].astype(F32)
        out_ref[:, :, cut] = (base + inc.reshape(L, TR, 256)).astype(BF16)

    bytes_wait(rs_ref, rs_send)
    bytes_wait(y_ref, y_send)
    bytes_wait(z_ref, z_send)
    bytes_wait(all_ref.at[pl.ds(0, 7)], ag_send)

    @pl.when(jnp.logical_not(is_parent))
    def _():
        bytes_wait(gat_ref.at[pl.ds(0, NR - 1)], g_send)
        bytes_wait(win_ref, w_send)


def per_device(fields, offset, level_index, nudge_rate, driving):
    smem = pl.BlockSpec(memory_space=pltpu.SMEM)
    vmem = pl.BlockSpec(memory_space=pltpu.VMEM)
    dma = pltpu.SemaphoreType.DMA
    out = pl.pallas_call(
        kernel,
        out_shape=jax.ShapeDtypeStruct((L, TR, TC), BF16),
        in_specs=[pl.BlockSpec(memory_space=pl.ANY), smem, smem, smem, vmem],
        out_specs=vmem,
        scratch_shapes=[
            pltpu.VMEM((L, TR, TC), BF16),
            pltpu.VMEM((TC, 256), BF16),
            pltpu.VMEM((2, L * TR, 128), F32),
            pltpu.VMEM((L, 16, 256), F32),
            pltpu.VMEM((L, 16, 256), BF16),
            pltpu.VMEM((B, TC), BF16),
            pltpu.VMEM((8, 16, 128), F32),
            pltpu.VMEM((7, 16, 128), F32),
            pltpu.VMEM((16, 128), F32),
            pltpu.VMEM((7, 16, 128), F32),
            pltpu.VMEM((16, 128), F32),
            pltpu.VMEM((7, 16, 128), F32),
            pltpu.VMEM((8, 16, 128), F32),
            pltpu.VMEM((NR, 2, 16, 256), BF16),
            pltpu.VMEM((2, 2, TR, 256), BF16),
            pltpu.VMEM((3, 2, 2, TR, 256), BF16),
            pltpu.VMEM((8, 16, 128), F32),
            pltpu.VMEM((TR, 3 * B), BF16),
            pltpu.VMEM((256, TC), BF16),
            pltpu.VMEM((256, TC), BF16),
        ]
        + [dma] * 13,
        compiler_params=pltpu.CompilerParams(collective_id=0, has_side_effects=True),
    )(fields[0], offset, level_index, nudge_rate, driving)
    return out[None]


def solution(mesh):
    spec = P("grp", None, "row", "col")
    return jax.shard_map(
        per_device, mesh=mesh, in_specs=(spec, P(), P(), P(), P()), out_specs=spec, check_vma=False
    )
```

```python
import math

import jax
import jax.numpy as jnp
from jax import lax
from jax.experimental import pallas as pl
from jax.experimental.pallas import tpu as pltpu
from jax.sharding import PartitionSpec as P

MESH = pl.DeviceIdType.MESH
F32 = jnp.float32
BF16 = jnp.bfloat16
I32 = jnp.int32

L = 4
W = 32
B = 64
ROWS = 768
COLS = 6144
TR = 48
TC = 768
NX = 4
NY = 8
NZ = 8
NR = 16
FAR_FIRST = (4, 3, 5, 2, 6, 1, 7)


def iota(shape, dim):
    return lax.broadcasted_iota(I32, shape, dim)


def basis(m, z, cells):
    period = 3 * cells
    wave = jnp.where(m <= W, m, m - W).astype(F32)
    shift = jnp.where(m <= W, 0.0, period / 4).astype(F32)
    scale = jnp.where(m == 0, 1.0 / math.sqrt(cells), math.sqrt(2.0 / cells)).astype(F32)
    phase = wave * z.astype(F32) - shift
    phase = phase - period * jnp.floor(phase * (1.0 / period))
    t = (jnp.abs(phase - period / 2) - period / 4) * (2.0 * math.pi / period)
    s = t * t
    acc = F32(1.0 / math.factorial(13))
    for k in (11, 9, 7, 5, 3, 1):
        sign = -1.0 if k in (11, 7, 3) else 1.0
        acc = acc * s + F32(sign / math.factorial(k))
    return scale * (t * acc)


def split(v):
    hi = v.astype(BF16)
    return hi, (v - hi.astype(F32)).astype(BF16)


def dot(a, b):
    return jnp.dot(a, b, preferred_element_type=F32)


def dot_nt(a, b):
    return lax.dot_general(a, b, (((1,), (1,)), ((), ())), preferred_element_type=F32)


def bytes_wait(ref, sem):
    pltpu.make_async_copy(ref, ref, sem).wait()


def kernel(
    x_hbm, off_ref, lev_hbm, rate_hbm, drv_hbm, out_ref,
    lev_ref, rate_ref, drv_ref, x_ref, pool_ref, sums_ref, avg_ref, own_ref, colt_ref, part_ref, rs_ref, ysrc_ref, y_ref,
    zsrc_ref, z_ref, all_ref, gat_ref, win_ref, fed_ref, drvp_ref, rows3_ref, chi_ref, clo_ref,
    in_sem, lev_sem, rate_sem, drv_sem, rs_send, rs_recv, y_send, y_recv, z_send, z_recv, ag_send, ag_recv,
    g_send, g_recv, w_send, w_recv,
):
    grp = lax.axis_index("grp")
    row = lax.axis_index("row")
    col = lax.axis_index("col")
    zed = row // 2
    core = row % 2
    seat = grp * 2 + core
    is_parent = grp == NX - 1
    load = pltpu.make_async_copy(x_hbm, x_ref, in_sem)
    load.start()
    load_lev = pltpu.make_async_copy(lev_hbm, lev_ref, lev_sem)
    load_rate = pltpu.make_async_copy(rate_hbm, rate_ref, rate_sem)
    load_drv = pltpu.make_async_copy(drv_hbm, drv_ref, drv_sem)
    load_lev.start()
    load_rate.start()
    load_drv.start()

    barrier = pltpu.get_barrier_semaphore()

    def seat_peer(d):
        other = (seat + d) % 8
        return other, (other // 2, zed * 2 + other % 2, col)

    def y_peer(d):
        return (grp, row, (col + d) % NY)

    def z_peer(d):
        return (grp, ((zed + d) % NZ) * 2 + core, col)

    def greet(dev):
        pl.semaphore_signal(barrier, inc=1, device_id=dev, device_id_type=MESH)

    for d in FAR_FIRST:
        greet(seat_peer(d)[1])
    for d in FAR_FIRST:
        greet(y_peer(d))
        greet(z_peer(d))

    @pl.when(jnp.logical_not(is_parent))
    def _():
        for d in FAR_FIRST:
            greet((grp, ((zed + d) % NZ) * 2 + 1 - core, col))

    @pl.when(jnp.logical_not(is_parent))
    def _():
        j = iota((TC, 256), 0)
        t = iota((TC, 256), 1) * 3
        pool_ref[...] = jnp.where((j >= t) & (j < t + 3), 1.0, 0.0).astype(BF16)
        xs = 3 * (col * TC + grp * 256 + iota((B, 256), 1))
        colt_ref[:, :256] = basis(iota((B, 256), 0), xs, COLS).astype(BF16)

    @pl.when(is_parent)
    def _():
        xs = 3 * (col * TC + iota((B, TC), 1))
        colt_ref[...] = basis(iota((B, TC), 0), xs, COLS).astype(BF16)

    load_lev.wait()
    off = off_ref[0]
    load.wait()

    def add_part(rowt, proj, rows):
        for pair in range(2):
            lo = 2 * pair * rows
            both = jnp.concatenate([proj[lo : lo + rows], proj[lo + rows : lo + 2 * rows]], axis=1)
            hi, low = split(both)
            part = dot(rowt, hi) + dot(rowt, low)
            part = part.reshape(4, 2, 8, 128)
            for h in range(2):
                part_ref[h, 4 * pair : 4 * pair + 4] = part[:, h]

    @pl.when(jnp.logical_not(is_parent))
    def _():
        xs = x_ref[...].reshape(L * TR, TC)
        for h in range(2):
            cut = slice(128 * h, 128 * h + 128)
            sums_ref[h] = dot(xs, pool_ref[:, cut])
            total = (
                sums_ref[h, pl.ds(0, 64, stride=3), :]
                + sums_ref[h, pl.ds(1, 64, stride=3), :]
                + sums_ref[h, pl.ds(2, 64, stride=3), :]
            )
            avg_ref[:, :, cut] = (total / 9.0).reshape(L, 16, 128)
        for p in range(L):
            inv = jnp.int32(0)
            for l in range(1, L):
                inv = jnp.where(lev_ref[l] == p, l, inv)
            own_ref[p] = avg_ref[inv].astype(BF16)
        proj = dot_nt(own_ref[...].reshape(64, 256), colt_ref[:, :256])
        rr = off + 16 * row + iota((B, 16), 1)
        rowt = basis(iota((B, 16), 0), 3 * rr, ROWS).astype(BF16)
        add_part(rowt, proj, 16)

    @pl.when(is_parent)
    def _():
        proj = dot_nt(x_ref[...].reshape(L * TR, TC), colt_ref[...])
        rr = TR * row + iota((B, TR), 1)
        s = rr - off
        s = jnp.where(s < 0, s + ROWS, s)
        rowt = basis(iota((B, TR), 0), 3 * rr, ROWS)
        rowt = jnp.where(s < ROWS // 3, 0.0, rowt).astype(BF16)
        add_part(rowt, proj, TR)

    pl.semaphore_wait(barrier, jnp.where(is_parent, 21, 28))

    def send(src, dst, sems, h, dev):
        pltpu.make_async_remote_copy(
            src_ref=src, dst_ref=dst, send_sem=sems[0].at[h], recv_sem=sems[1].at[h],
            device_id=dev, device_id_type=MESH,
        ).start()

    for h in range(2):
        for d in FAR_FIRST:
            other, dev = seat_peer(d)
            send(part_ref.at[h, other], rs_ref.at[h, d - 1], (rs_send, rs_recv), h, dev)

    @pl.when(jnp.logical_not(is_parent))
    def _():
        for d in range(1, NR):
            other = (row + d) % NR
            pltpu.make_async_remote_copy(
                src_ref=own_ref.at[pl.ds(2 * (other % 2), 2)], dst_ref=gat_ref.at[row],
                send_sem=g_send, recv_sem=g_recv, device_id=(grp, other, col), device_id_type=MESH,
            ).start()
        gat_ref[row] = own_ref[pl.ds(2 * core, 2)]

    load_drv.wait()
    load_rate.wait()
    for pair in range(2):
        both = jnp.concatenate([drv_ref[2 * pair], drv_ref[2 * pair + 1]], axis=1)
        both = (both * (math.sqrt(ROWS * COLS) / (2 * W))).reshape(4, 2, 8, 128)
        for h in range(2):
            drvp_ref[h, 4 * pair : 4 * pair + 4] = both[:, h]
    t = iota((TR, B), 0)
    zr = jnp.where(is_parent, 3 * (TR * row + t), 3 * off + TR * row + t - 1)
    hi, low = split(basis(iota((TR, B), 1), zr, ROWS))
    rows3_ref[...] = jnp.concatenate([hi, hi, low], axis=1)

    def summed(own, got, h):
        total = own
        for d in range(7):
            total = total + got[h, d]
        return total

    for h in range(2):
        bytes_wait(rs_ref.at[h], rs_recv.at[h])
        ysrc_ref[h] = summed(part_ref[h, seat], rs_ref, h)
        for d in FAR_FIRST:
            send(ysrc_ref.at[h], y_ref.at[h, d - 1], (y_send, y_recv), h, y_peer(d))

    for n in range(3):
        t = iota((B, 256), 1) + 256 * n
        zc = jnp.where(is_parent, 3 * (col * TC + t), (3 * col + grp) * TC + t - 1)
        hi, low = split(basis(iota((B, 256), 0), zc, COLS))
        for p in range(L):
            chi_ref[p * B : (p + 1) * B, n * 256 : (n + 1) * 256] = hi
            clo_ref[p * B : (p + 1) * B, n * 256 : (n + 1) * 256] = low

    @pl.when(is_parent)
    def _():
        s = TR * row + iota((TR, TC), 0) - off
        s = jnp.where(s < 0, s + ROWS, s)
        for p in range(L):
            x_ref[p] = jnp.where(s < ROWS // 3, 0.0, x_ref[p].astype(F32)).astype(BF16)

    for h in range(2):
        bytes_wait(y_ref.at[h], y_recv.at[h])
        zsrc_ref[h] = summed(ysrc_ref[h], y_ref, h)
        for d in FAR_FIRST:
            send(zsrc_ref.at[h], z_ref.at[h, d - 1], (z_send, z_recv), h, z_peer(d))

    @pl.when(jnp.logical_not(is_parent))
    def _():
        bytes_wait(gat_ref.at[pl.ds(0, NR - 1)], g_recv)
        v = 2 * TR * zed + iota((2 * TR, 256), 0) - off
        q = iota((2 * TR, 256), 1)
        pick = jnp.where((v == q) | (v + ROWS == q), 1.0, 0.0).astype(BF16)
        for k in range(2):
            rows = dot(pick, gat_ref[:, k].reshape(256, 256)).astype(BF16)
            win_ref[0, k] = rows[:TR]
            win_ref[1, k] = rows[TR:]
        for k in range(2):
            pltpu.make_async_remote_copy(
                src_ref=win_ref.at[k], dst_ref=fed_ref.at[grp, core], send_sem=w_send, recv_sem=w_recv,
                device_id=(NX - 1, 2 * zed + k, col), device_id_type=MESH,
            ).start()

    for h in range(2):
        bytes_wait(z_ref.at[h], z_recv.at[h])
        all_ref[h, seat] = drvp_ref[h, seat] - summed(zsrc_ref[h], z_ref, h)
        for d in FAR_FIRST:
            mine = all_ref.at[h, seat]
            send(mine, mine, (ag_send, ag_recv), h, seat_peer(d)[1])
    for h in range(2):
        bytes_wait(all_ref.at[h, pl.ds(0, 7)], ag_recv.at[h])

    whole = jnp.stack([all_ref[0], all_ref[1]], axis=1).reshape(2, B, 128)
    hi, low = split(jnp.concatenate([whole[0], whole[1]], axis=1))
    left = dot(rows3_ref[...], jnp.concatenate([hi, low, hi], axis=0))
    slot = iota((TR, 256), 1) // B
    parts = []
    for l in range(L):
        lev = jnp.where(is_parent, l, lev_ref[l])
        parts.append(jnp.where(slot == lev, left * rate_ref[lev], 0.0))
    lhi, llow = split(jnp.concatenate(parts, axis=0))

    @pl.when(is_parent)
    def _():
        bytes_wait(fed_ref, w_recv)
        for g in range(3):
            for p in range(L):
                cut = (p, slice(None), slice(256 * g, 256 * g + 256))
                x_ref[cut] = x_ref[cut] + fed_ref[g, p // 2, p % 2]

    for n in range(3):
        cut = slice(n * 256, n * 256 + 256)
        inc = dot(lhi, chi_ref[:, cut]) + dot(lhi, clo_ref[:, cut]) + dot(llow, chi_ref[:, cut])
        base = x_ref[:, :, cut].astype(F32)
        out_ref[:, :, cut] = (base + inc.reshape(L, TR, 256)).astype(BF16)

    for h in range(2):
        bytes_wait(rs_ref.at[h], rs_send.at[h])
        bytes_wait(y_ref.at[h], y_send.at[h])
        bytes_wait(z_ref.at[h], z_send.at[h])
        bytes_wait(all_ref.at[h, pl.ds(0, 7)], ag_send.at[h])

    @pl.when(jnp.logical_not(is_parent))
    def _():
        bytes_wait(gat_ref.at[pl.ds(0, NR - 1)], g_send)
        bytes_wait(win_ref, w_send)


def per_device(fields, offset, level_index, nudge_rate, driving):
    anywhere = pl.BlockSpec(memory_space=pltpu.HBM)
    dma = pltpu.SemaphoreType.DMA
    out = pl.pallas_call(
        kernel,
        out_shape=pltpu.VMEM((L, TR, TC), BF16),
        in_specs=[anywhere, pl.BlockSpec(memory_space=pltpu.SMEM)] + [anywhere] * 3,
        out_specs=pl.BlockSpec(memory_space=pltpu.VMEM),
        scratch_shapes=[
            pltpu.SMEM((L,), I32),
            pltpu.SMEM((L,), F32),
            pltpu.VMEM((L, B, B), F32),
            pltpu.VMEM((L, TR, TC), BF16),
            pltpu.VMEM((TC, 256), BF16),
            pltpu.VMEM((2, L * TR, 128), F32),
            pltpu.VMEM((L, 16, 256), F32),
            pltpu.VMEM((L, 16, 256), BF16),
            pltpu.VMEM((B, TC), BF16),
            pltpu.VMEM((2, 8, 8, 128), F32),
            pltpu.VMEM((2, 7, 8, 128), F32),
            pltpu.VMEM((2, 8, 128), F32),
            pltpu.VMEM((2, 7, 8, 128), F32),
            pltpu.VMEM((2, 8, 128), F32),
            pltpu.VMEM((2, 7, 8, 128), F32),
            pltpu.VMEM((2, 8, 8, 128), F32),
            pltpu.VMEM((NR, 2, 16, 256), BF16),
            pltpu.VMEM((2, 2, TR, 256), BF16),
            pltpu.VMEM((3, 2, 2, TR, 256), BF16),
            pltpu.VMEM((2, 8, 8, 128), F32),
            pltpu.VMEM((TR, 3 * B), BF16),
            pltpu.VMEM((256, TC), BF16),
            pltpu.VMEM((256, TC), BF16),
        ]
        + [dma] * 4
        + [dma((2,))] * 8
        + [dma] * 4,
        compiler_params=pltpu.CompilerParams(
            collective_id=0, has_side_effects=True
        ),
    )(fields[0], offset, level_index, nudge_rate, driving)
    return out[None]


def solution(mesh):
    spec = P("grp", None, "row", "col")
    return jax.shard_map(
        per_device, mesh=mesh, in_specs=(spec, P(), P(), P(), P()), out_specs=spec, check_vma=False
    )
```
